1024 devices in a mesh: node: 32 (over z_lo, y, core), rep: 32 (over x, z_hi).
Axes of the slice: x: 8, y: 8, z: 8 (z_hi: 4, z_lo: 2; z = z_hi * 2 + z_lo), core: 2. Of those that a mesh axis runs over, the one named last changes fastest.
Arguments:
- tokens: bfloat16 [262144, 2048], P(('node', 'rep')), may hold values from -60 to 60
- cotangent: bfloat16 [262144, 512], P(('node', 'rep')), may hold values from -6 to 6
- value_weight: bfloat16 [2048, 512], P('node'), may hold values from -0.25 to 0.25
Outputs:
- input_grad: bfloat16 [262144, 2048], P(('node', 'rep'))
- update: float32 [2048, 512], P('node')
The draws below stay inside these ranges and needn't reach their ends.
All inputs are finite; a program needn't handle non-finite values.
Results may differ from the reference program's by a relative error of at most 0.025.
Values may be sent and summed in bfloat16 or wider, within the bound.
A program may use at most 32 MiB of HBM per device.

```python
import math
import jax
import jax.numpy as jnp
from jax import lax

DIN = 2048
KVH = 4
HD = 128
NS_ITERS = 5
TOK_DEV = 256
CV = 512
TOKENS = 262144
N_NODE = 32


def draw_tokens(key, part):
    key_values = jax.random.fold_in(key, 11)
    key_rough = jax.random.fold_in(key, 12)
    key_pair = jax.random.fold_in(key, 13)
    columns = jnp.arange(DIN, dtype=jnp.float32) / (DIN - 1)
    rough = jnp.exp(jax.random.uniform(key_rough, (DIN,), jnp.float32, jnp.log(0.7), jnp.log(1.4)))
    values = jnp.clip(jax.random.normal(key_values, (TOKENS, DIN), jnp.float32), -6.0, 6.0)
    rise = 3.0 ** columns
    offset = jax.random.randint(key_pair, (), 0, N_NODE)
    row_block = jnp.arange(TOKENS, dtype=jnp.int32) // TOK_DEV
    col_block = jnp.arange(DIN, dtype=jnp.int32) // (DIN // N_NODE)
    paired = ((row_block + offset) % N_NODE)[:, None] == col_block[None, :]
    spike = jnp.where(paired, 3.0, 1.0).astype(jnp.float32)
    return (values * spike * (rise * rough)[None, :]).astype(jnp.bfloat16)


def shard_levels(own_key, dims, pieces, smallest, high):
    loudness, own = 1.0, jax.random.fold_in(own_key, 6)
    for position, shards_of in pieces:
        draws = jnp.exp(jax.random.uniform(jax.random.fold_in(own, position), (shards_of,), jnp.float32, smallest / len(pieces), high / len(pieces)))
        loudness = loudness * jnp.repeat(draws, dims[position] // shards_of).reshape([-1 if axis == position else 1 for axis in range(len(dims))])
    return loudness


def noise(key, extent, deviation, most, split=(), kind=jnp.bfloat16):
    drawn = jax.random.normal(key, extent, jnp.float32) * deviation
    if len(split) > 0:
        drawn = shard_levels(key, extent, split, -0.22, 0.18) * drawn
    return jnp.clip(drawn, min=-most, max=most).astype(kind)


def setup_inputs(seed: int = 0) -> dict:
    seeds = jax.random.split(jax.random.key(seed), 4)
    tokens = draw_tokens(jax.random.fold_in(seeds[3], 71), 0)
    cotangent = noise(seeds[1], (TOKENS, CV), 1.0, 6.0, ((0, 1024),))
    value_weight = noise(seeds[2], (DIN, CV), CV ** -0.5, 0.25, ((0, 32),))
    return {"tokens": tokens, "cotangent": cotangent, "value_weight": value_weight}


coef_a = 3.4445
coef_b = -4.775
coef_c = 2.0315
epsilon = 1e-07

def block_term(total, pair):
    rows_x, rows_c = pair
    term = jnp.einsum('td,tc->dc', rows_x.astype(jnp.float32), rows_c.astype(jnp.float32), precision=lax.Precision.HIGHEST)
    rounded = lax.optimization_barrier(term.astype(jnp.bfloat16))
    return (total + rounded.astype(jnp.float32), None)

def reference(tokens, cotangent, value_weight):
    width = cotangent.shape[1]
    input_grad = jnp.dot(cotangent, value_weight.T, preferred_element_type=jnp.float32).astype(jnp.bfloat16)
    blocks_x = tokens.reshape(-1, TOK_DEV, DIN)
    blocks_c = cotangent.reshape(-1, TOK_DEV, width)
    gradient, unused = lax.scan(block_term, jnp.zeros((DIN, width), jnp.float32), (blocks_x, blocks_c))
    blocks = gradient.reshape(DIN, KVH, HD)
    norms = jnp.sqrt(lax.optimization_barrier(jnp.sum(blocks * blocks, axis=(0, 2))))
    iterate = blocks / (norms[None, :, None] + epsilon)
    for step in range(NS_ITERS):
        gram = jnp.einsum('rhi,rhj->hij', iterate, iterate, precision=lax.Precision.HIGHEST)
        poly = coef_b * gram + coef_c * jnp.einsum('hij,hjk->hik', gram, gram, precision=lax.Precision.HIGHEST)
        iterate = coef_a * iterate + jnp.einsum('rhi,hij->rhj', iterate, poly, precision=lax.Precision.HIGHEST)
    update = 0.2 * math.sqrt(DIN) * iterate.reshape(DIN, width)
    return (input_grad, update)
```

```python
import functools
import math

import jax
import jax.numpy as jnp
from jax import lax
from jax.experimental import pallas as pl
from jax.experimental.pallas import tpu as pltpu
from jax.sharding import PartitionSpec as P

MESH = pl.DeviceIdType.MESH

DIN = 2048
HD = 128
NS_ITERS = 5

coef_a = 3.4445
coef_b = -4.775
coef_c = 2.0315
epsilon = 1e-07

NX, NY, NZ, NZH = 8, 8, 8, 4
FAR = (4, 3, 5, 2, 6, 1, 7)


def mm(a, b):
    return jnp.dot(a, b, precision=lax.Precision.HIGHEST, preferred_element_type=jnp.float32)


def kernel(
    tok_hbm, cot_hbm, w_hbm, ig_hbm, up_ref,
    tok, cot, wfull, ig,
    term, other, px, py, rx, ry, sx, sy, r2x, r2y,
    qz, rz, gh, af, rc, bslice, rg, gram, ub,
    load_sem, out_sem, d2d_s, d2d_r, w1_s, w1_r, w2_s, w2_r, w3_s, w3_r,
    x1_s, x1_r, y1_s, y1_r, x2_s, x2_r, y2_s, y2_r, z_s, z_r, g_s, g_r,
    c_s, c_r, b_s, b_r, a_s, a_r, u_s, u_r,
):
    node, rep = lax.axis_index("node"), lax.axis_index("rep")
    core = lax.rem(node, 2)
    y = lax.rem(lax.div(node, 2), NY)
    zl = lax.div(node, 2 * NY)
    x, zh = lax.div(rep, NZH), lax.rem(rep, NZH)
    z = zh * 2 + zl

    def dev(x_=None, y_=None, z_=None, core_=None):
        x_ = x if x_ is None else x_
        y_ = y if y_ is None else y_
        z_ = z if z_ is None else z_
        core_ = core if core_ is None else core_
        zl_, zh_ = lax.rem(z_, 2), lax.div(z_, 2)
        return {"node": (zl_ * NY + y_) * 2 + core_, "rep": x_ * NZH + zh_}

    def ahead(at, d, n):
        return lax.rem(at + d, n)

    def send(src, dst, ssem, rsem, to):
        copy = pltpu.make_async_remote_copy(
            src_ref=src, dst_ref=dst, send_sem=ssem, recv_sem=rsem, device_id=to, device_id_type=MESH
        )
        copy.start()
        return copy

    z_pair = z + 1 - 2 * zl
    partner = dev(core_=1 - core)

    barrier = pltpu.get_barrier_semaphore()
    peers = [dev(x_=ahead(x, d, NX)) for d in FAR]
    peers += [dev(y_=ahead(y, d, NY)) for d in FAR]
    peers += [dev(z_=ahead(z, d, NZ)) for d in FAR]
    peers += [partner, dev(z_=z_pair, core_=1 - core)]
    for to in peers:
        pl.semaphore_signal(barrier, inc=1, device_id=to, device_id_type=MESH)

    load_cot = pltpu.make_async_copy(cot_hbm, cot, load_sem.at[0])
    load_cot.start()
    loads = []
    for k in range(8):
        columns = pl.ds((k % 2) * 1024 + (k // 2) * 256, 256)
        load = pltpu.make_async_copy(tok_hbm.at[:, columns], tok.at[:, columns], load_sem.at[2 + k])
        load.start()
        loads.append(load)
    load_w = pltpu.make_async_copy(w_hbm.at[zh], wfull.at[zl, y, core, zh], load_sem.at[1])
    load_w.start()

    unsent = []
    load_cot.wait()
    d2d = []
    for k in range(4):
        halves = []
        for lo in range(2):
            loads[2 * k + lo].wait()
            t = lax.dot_general(
                tok[:, lo * 1024 + k * 256 : lo * 1024 + k * 256 + 256],
                cot[...],
                (((0,), (0,)), ((), ())),
                preferred_element_type=jnp.float32,
            )
            halves.append(t.reshape(2, 2, 8, 8, 512))
        term[2 * k : 2 * k + 2] = jnp.concatenate(halves, axis=3).astype(jnp.bfloat16)
        if k == 0:
            pl.semaphore_wait(barrier, len(peers))
        d2d.append(
            send(term.at[pl.ds(2 * k, 2), 1 - core], other.at[pl.ds(2 * k, 2)], d2d_s.at[k], d2d_r.at[k], partner)
        )
    unsent += d2d

    load_w.wait()
    w1 = []
    for i, d in enumerate(FAR):
        mine = wfull.at[zl, y, core, zh]
        w1.append(send(mine, mine, w1_s.at[i], w1_r.at[i], dev(y_=ahead(y, d, NY))))
    unsent += w1

    for k in range(4):
        d2d[k].wait_recv()
        for b in (2 * k, 2 * k + 1):
            s = term[b, core].astype(jnp.float32) + other[b].astype(jnp.float32)
            s = s.astype(jnp.bfloat16)
            px[:, b] = s[:, :, :256]
            py[b] = s[:, :, 256:]

    first = []
    for i, d in enumerate(FAR):
        to_x, to_y = ahead(x, d, NX), ahead(y, d, NY)
        first.append(send(px.at[to_x], rx.at[i], x1_s.at[i], x1_r.at[i], dev(x_=to_x)))
        first.append(send(py.at[to_y], ry.at[i], y1_s.at[i], y1_r.at[i], dev(y_=to_y)))
    unsent += first

    for copy in w1:
        copy.wait_recv()
    w2 = []
    for i, d in enumerate(FAR):
        mine = wfull.at[zl, :, core, zh]
        w2.append(send(mine, mine, w2_s.at[i], w2_r.at[i], dev(z_=ahead(z, d, NZ))))
    unsent += w2

    for copy in first:
        copy.wait_recv()
    for b in range(8):
        total_x = px[x, b].astype(jnp.float32)
        total_y = py[y, b].astype(jnp.float32)
        for i in range(7):
            total_x += rx[i, b].astype(jnp.float32)
            total_y += ry[i, b].astype(jnp.float32)
        sx[b] = total_x.astype(jnp.bfloat16)
        sy[b] = total_y.astype(jnp.bfloat16)

    second = []
    for i, d in enumerate(FAR):
        to_x, to_y = ahead(x, d, NX), ahead(y, d, NY)
        second.append(send(sx.at[to_y], r2x.at[i], y2_s.at[i], y2_r.at[i], dev(y_=to_y)))
        second.append(send(sy.at[to_x], r2y.at[i], x2_s.at[i], x2_r.at[i], dev(x_=to_x)))
    unsent += second
    for copy in second:
        copy.wait_recv()
    total_x = sx[y].astype(jnp.float32)
    total_y = sy[x].astype(jnp.float32)
    for i in range(7):
        total_x += r2x[i].astype(jnp.float32)
        total_y += r2y[i].astype(jnp.float32)
    for lo in range(2):
        for h in range(4):
            source = total_x if h < 2 else total_y
            qz[lo, h] = source[8 * lo : 8 * lo + 8, (h % 2) * HD : (h % 2) * HD + HD]

    third = []
    for i, d in enumerate(FAR):
        to_z = ahead(z, d, NZ)
        third.append(
            send(qz.at[lax.rem(to_z, 2), lax.div(to_z, 2)], rz.at[i], z_s.at[i], z_r.at[i], dev(z_=to_z))
        )
    unsent += third
    for copy in third:
        copy.wait_recv()
    rows = qz[zl, zh]
    for i in range(7):
        rows += rz[i]
    gh[x] = rows

    gather = []
    for i, d in enumerate(FAR):
        gather.append(send(gh.at[x], gh.at[x], g_s.at[i], g_r.at[i], dev(x_=ahead(x, d, NX))))
    unsent += gather
    for copy in gather:
        copy.wait_recv()

    g = gh[...].reshape(64, HD)
    partial = lax.dot_general(
        g, g, (((0,), (0,)), ((), ())), precision=lax.Precision.HIGHEST, preferred_element_type=jnp.float32
    )
    af[...] = partial.reshape(8, 16, HD)

    quad = [
        send(af.at[x], rc.at[0], c_s.at[0], c_r.at[0], partner),
        send(af.at[x], rc.at[1], c_s.at[1], c_r.at[1], dev(z_=z_pair)),
        send(af.at[x], rc.at[2], c_s.at[2], c_r.at[2], dev(z_=z_pair, core_=1 - core)),
    ]
    unsent += quad
    for copy in quad:
        copy.wait_recv()
    bslice[...] = af[x] + rc[0] + rc[1] + rc[2]

    over_y = []
    for i, d in enumerate(FAR):
        over_y.append(send(bslice, rg.at[i], b_s.at[i], b_r.at[i], dev(y_=ahead(y, d, NY))))
    unsent += over_y

    for copy in w2:
        copy.wait_recv()
    w3 = send(wfull.at[:, :, core], wfull.at[:, :, core], w3_s, w3_r, partner)
    unsent.append(w3)

    for copy in over_y:
        copy.wait_recv()
    total = bslice[...]
    for i in range(7):
        total += rg[i]
    gram[x] = total

    over_x = []
    for i, d in enumerate(FAR):
        over_x.append(send(gram.at[x], gram.at[x], a_s.at[i], a_r.at[i], dev(x_=ahead(x, d, NX))))
    unsent += over_x

    w3.wait_recv()
    outs = []
    for k in range(8):
        lo, b = k // 4, 2 * (k % 4)
        weight = wfull[lo, b : b + 2].reshape(256, 512)
        ig[:, k * 256 : k * 256 + 256] = lax.dot_general(
            cot[...], weight, (((1,), (1,)), ((), ())), preferred_element_type=jnp.float32
        ).astype(jnp.bfloat16)
        columns = pl.ds(k * 256, 256)
        out = pltpu.make_async_copy(ig.at[:, columns], ig_hbm.at[:, columns], out_sem.at[k])
        out.start()
        outs.append(out)

    for copy in over_x:
        copy.wait_recv()
    a = gram[...].reshape(HD, HD)
    row = lax.broadcasted_iota(jnp.int32, (HD, HD), 0)
    col = lax.broadcasted_iota(jnp.int32, (HD, HD), 1)
    eye = row == col
    identity = jnp.where(eye, 1.0, 0.0).astype(jnp.float32)
    square = jnp.sum(jnp.where(eye, a, 0.0), axis=0, keepdims=True)
    square = jnp.sum(square, axis=1, keepdims=True)
    divisor = jnp.sqrt(square) + epsilon
    a = a / (divisor * divisor)
    total = None
    for step in range(NS_ITERS):
        factor = coef_a * identity + coef_b * a + coef_c * mm(a, a)
        total = factor if total is None else mm(total, factor)
        if step + 1 < NS_ITERS:
            a = mm(factor, mm(a, factor))
    ub[zh] = (0.2 * math.sqrt(DIN)) * mm(gh[...].reshape(64, HD) / divisor, total)

    last = []
    for d in (1, 2, 3):
        to_z = lax.rem(zh + d, NZH) * 2 + zl
        last.append(send(ub.at[zh], ub.at[zh], u_s.at[d - 1], u_r.at[d - 1], dev(z_=to_z)))
    unsent += last
    for copy in last:
        copy.wait_recv()
    for h in range(4):
        up_ref[:, h * HD : h * HD + HD] = ub[h]

    for copy in unsent:
        copy.wait_send()
    for out in outs:
        out.wait()


def per_device(tokens, cotangent, value_weight):
    bf16, f32 = jnp.bfloat16, jnp.float32
    vmem, dma = pltpu.VMEM, pltpu.SemaphoreType.DMA
    seven = [dma((7,)), dma((7,))]
    return pl.pallas_call(
        kernel,
        out_shape=(
            jax.ShapeDtypeStruct((256, DIN), bf16),
            jax.ShapeDtypeStruct((64, 512), f32),
        ),
        in_specs=[pl.BlockSpec(memory_space=pl.ANY)] * 3,
        out_specs=(pl.BlockSpec(memory_space=pl.ANY), pl.BlockSpec(memory_space=pltpu.VMEM)),
        scratch_shapes=[
            vmem((256, DIN), bf16),
            vmem((256, 512), bf16),
            vmem((2, NY, 2, NZH, 16, 512), bf16),
            vmem((256, DIN), bf16),
            vmem((8, 2, 8, 16, 512), bf16),
            vmem((8, 8, 16, 512), bf16),
            vmem((8, 8, 16, 256), bf16),
            vmem((8, 8, 16, 256), bf16),
            vmem((7, 8, 16, 256), bf16),
            vmem((7, 8, 16, 256), bf16),
            vmem((8, 16, 256), bf16),
            vmem((8, 16, 256), bf16),
            vmem((7, 16, 256), bf16),
            vmem((7, 16, 256), bf16),
            vmem((2, 4, 8, HD), f32),
            vmem((7, 8, HD), f32),
            vmem((8, 8, HD), f32),
            vmem((8, 16, HD), f32),
            vmem((3, 16, HD), f32),
            vmem((16, HD), f32),
            vmem((7, 16, HD), f32),
            vmem((8, 16, HD), f32),
            vmem((4, 64, HD), f32),
            dma((10,)), dma((8,)), dma((4,)), dma((4,)),
            *seven, *seven, dma, dma,
            *seven, *seven, *seven, *seven, *seven, *seven,
            dma((3,)), dma((3,)), *seven, *seven, dma((3,)), dma((3,)),
        ],
        compiler_params=pltpu.CompilerParams(
            collective_id=0, has_side_effects=True, vmem_limit_bytes=60 * 1024 * 1024
        ),
        name="whole",
    )(tokens, cotangent, value_weight.reshape(NZH, 16, 512))


def solution(mesh):
    in_specs = (P(("node", "rep"), None), P(("node", "rep"), None), P("node", None))
    out_specs = (P(("node", "rep"), None), P("node", None))
    return jax.shard_map(
        per_device, mesh=mesh, in_specs=in_specs, out_specs=out_specs, check_vma=False
    )
```

```python
import functools
import math

import jax
import jax.numpy as jnp
from jax import lax
from jax.experimental import pallas as pl
from jax.experimental.pallas import tpu as pltpu
from jax.sharding import PartitionSpec as P

MESH = pl.DeviceIdType.MESH

DIN = 2048
HD = 128
NS_ITERS = 5

coef_a = 3.4445
coef_b = -4.775
coef_c = 2.0315
epsilon = 1e-07

NX, NY, NZ, NZH = 8, 8, 8, 4
FAR = (4, 3, 5, 2, 6, 1, 7)
EARLY, LATE = (3, 5, 2, 6), (4, 1, 7)
UPDATE_DTYPE = jnp.bfloat16
VMEM_LIMIT = 24 * 1024 * 1024


def mm(a, b):
    return jnp.dot(a, b, precision=lax.Precision.HIGHEST, preferred_element_type=jnp.float32)


def kernel(
    tok_hbm, cot_hbm, w_hbm, ig_ref, up_ref,
    tok, cot, wfull, wown,
    term, other, px, py, rx, ry, sx, sy, r2x, r2y,
    qz, rz, gh, af, rc, bslice, rg, gram, ub, uz,
    load_sem, d2d_s, d2d_r, w0_s, w0_r, w1_s, w1_r, w2_s, w2_r, w3_s, w3_r,
    x1_s, x1_r, y1_s, y1_r, x2_s, x2_r, y2_s, y2_r, z_s, z_r, g_s, g_r,
    c_s, c_r, b_s, b_r, a_s, a_r, u_s, v_s, u_r, go_sem,
):
    node, rep = lax.axis_index("node"), lax.axis_index("rep")
    core = lax.rem(node, 2)
    y = lax.rem(lax.div(node, 2), NY)
    zl = lax.div(node, 2 * NY)
    x, zh = lax.div(rep, NZH), lax.rem(rep, NZH)
    z = zh * 2 + zl

    def dev(x_=None, y_=None, z_=None, core_=None):
        to = {}
        if y_ is not None or z_ is not None or core_ is not None:
            low = zl if z_ is None else lax.rem(z_, 2)
            to["node"] = (low * NY + (y if y_ is None else y_)) * 2 + (core if core_ is None else core_)
        if x_ is not None or z_ is not None:
            to["rep"] = (x if x_ is None else x_) * NZH + (zh if z_ is None else lax.div(z_, 2))
        return to

    def ahead(at, d, n):
        return lax.rem(at + d, n)

    def describe(src, dst, ssem, rsem, to):
        return pltpu.make_async_remote_copy(
            src_ref=src, dst_ref=dst, send_sem=ssem, recv_sem=rsem, device_id=to, device_id_type=MESH
        )

    def send(src, dst, ssem, rsem, to):
        describe(src, dst, ssem, rsem, to).start()

    def wait(like, sem):
        pltpu.make_async_copy(like, like, sem).wait()

    partner = dev(core_=1 - core)

    load_cot = pltpu.make_async_copy(cot_hbm, cot, load_sem.at[0])
    load_cot.start()
    for k in range(4):
        for lo in range(2):
            columns = pl.ds(lo * 1024 + k * 256, 256)
            pltpu.make_async_copy(tok_hbm.at[:, columns], tok.at[:, columns], load_sem.at[2 + k]).start()
    load_w = pltpu.make_async_copy(w_hbm.at[zh], wown, load_sem.at[1])
    load_w.start()

    barrier = pltpu.get_barrier_semaphore()

    def greet(to):
        pl.semaphore_signal(barrier, inc=1, device_id=to, device_id_type=MESH)

    def z_hi_peer(d, core_):
        return dev(z_=lax.rem(zh + d, NZH) * 2 + zl, core_=core_)

    for d in FAR:
        greet(dev(z_=ahead(z, d, NZ)))

    @pl.when(core == 0)
    def _():
        for d in (2, 1, 3):
            greet(z_hi_peer(d, 1))

    for d in FAR:
        greet(dev(y_=ahead(y, d, NY)))

    @pl.when(core == 1)
    def _():
        for d in FAR:
            greet(dev(x_=ahead(x, d, NX)))

    greet(partner)

    def compute(k):
        wait(tok.at[:, pl.ds(0, 512)], load_sem.at[2 + k])
        for lo in range(2):
            t = lax.dot_general(
                tok[:, lo * 1024 + k * 256 : lo * 1024 + k * 256 + 256],
                cot[...],
                (((0,), (0,)), ((), ())),
                preferred_element_type=jnp.float32,
            )
            term[2 * k : 2 * k + 2, lo] = t.reshape(2, 8, 16, 512).astype(jnp.bfloat16)

    def piece(at):
        return wfull.at[lax.rem(at, 2), :, :, lax.div(at, 2)]

    def finish():
        for k in range(8):
            lo, b = k // 4, 2 * (k % 4)
            weight = wfull[lo, b : b + 2].reshape(256, 512)
            ig_ref[:, k * 256 : k * 256 + 256] = lax.dot_general(
                cot[...], weight, (((1,), (1,)), ((), ())), preferred_element_type=jnp.float32
            ).astype(jnp.bfloat16)

    def place():
        for h in range(4):
            up_ref[:, h * HD : h * HD + HD] = ub[h].astype(jnp.float32)

    to_partner = describe(wown, wfull.at[zl, y, 1, zh], w0_s, w0_r, partner)

    @pl.when(core == 0)
    def _():
        load_cot.wait()
        for k in range(4):
            compute(k)
            if k == 0:
                pl.semaphore_wait(barrier, 15)
            ys = pl.ds(2 * k, 2)
            send(term.at[ys], other.at[ys], d2d_s, d2d_r.at[k], partner)
            if k == 0:
                load_w.wait()
                wfull[zl, y, 0, zh] = wown[...]
            if k == 2:
                to_partner.wait_recv()
                mine = wfull.at[zl, y, :, zh]
                for d in FAR:
                    send(mine, mine, w1_s, w1_r, dev(y_=ahead(y, d, NY)))

        sevenths = wfull.at[0, pl.ds(0, 7), :, 0]
        four, three = wfull.at[0], wfull.at[0, :, :, pl.ds(0, 3)]
        wait(sevenths, w1_r)
        for d in EARLY:
            send(piece(z), piece(z), w2_s.at[0], w2_r.at[0], dev(z_=ahead(z, d, NZ)))
        send(piece(z), piece(z), w3_s, w3_r, partner)
        wait(four, w2_r.at[0])
        for d in EARLY:
            at = piece(lax.rem(z + NZ - d, NZ))
            send(at, at, w3_s, w3_r, partner)
        pl.semaphore_wait(go_sem, 1)
        for d in LATE:
            send(piece(z), piece(z), w2_s.at[1], w2_r.at[1], dev(z_=ahead(z, d, NZ)))
        wait(three, w2_r.at[1])
        for d in LATE:
            at = piece(lax.rem(z + NZ - d, NZ))
            send(at, at, w3_s, w3_r, partner)
        finish()
        wait(term, d2d_s)
        wait(sevenths, w1_s)
        wait(four, w2_s.at[0])
        wait(three, w2_s.at[1])
        wait(wfull, w3_s)
        wait(ub, u_r)
        place()

    @pl.when(core == 1)
    def _():
        load_cot.wait()
        compute(0)
        load_w.wait()
        pl.semaphore_wait(barrier, 25)
        to_partner.start()
        for k in range(1, 4):
            compute(k)

        for k in range(4):
            ys = pl.ds(2 * k, 2)
            wait(other.at[ys], d2d_r.at[k])
            for b in (2 * k, 2 * k + 1):
                for lo in range(2):
                    s = term[b, lo] + other[b, lo]
                    px[:, b, lo] = s[:, :, :256]
                    py[b, lo] = s[:, :, 256:]
            for b in (2 * k, 2 * k + 1):

                @pl.when(y != b)
                def _(b=b):
                    slot = lax.rem(b + NY - y, NY) - 1
                    send(py.at[b], ry.at[slot], y1_s, y1_r, dev(y_=b))

            if k % 2 == 1:
                ys = pl.ds(2 * k - 2, 4)
                for d in FAR:
                    to_x = ahead(x, d, NX)
                    send(px.at[to_x, ys], rx.at[d - 1, ys], x1_s, x1_r, dev(x_=to_x))

        wait(rx, x1_r)
        wait(ry, y1_r)
        for b in range(8):
            for lo in range(2):
                total_x = px[x, b, lo].astype(jnp.float32)
                total_y = py[y, lo, b].astype(jnp.float32)
                for i in range(7):
                    total_x += rx[i, b, lo].astype(jnp.float32)
                    total_y += ry[i, lo, b].astype(jnp.float32)
                sx[b, lo] = total_x.astype(jnp.bfloat16)
                sy[b, lo] = total_y.astype(jnp.bfloat16)

        for d in FAR:
            to_x, to_y = ahead(x, d, NX), ahead(y, d, NY)
            send(sx.at[to_y], r2x.at[d - 1], y2_s, y2_r, dev(y_=to_y))
            send(sy.at[to_x], r2y.at[d - 1], x2_s, x2_r, dev(x_=to_x))
        wait(r2x, y2_r)
        wait(r2y, x2_r)
        total_x = sx[y].astype(jnp.float32)
        total_y = sy[x].astype(jnp.float32)
        for i in range(7):
            total_x += r2x[i].astype(jnp.float32)
            total_y += r2y[i].astype(jnp.float32)
        for h in range(4):
            source = total_x if h < 2 else total_y
            qz[:, h] = source[:, :, (h % 2) * HD : (h % 2) * HD + HD]

        for d in FAR:
            to_z = ahead(z, d, NZ)
            send(qz.at[lax.rem(to_z, 2), lax.div(to_z, 2)], rz.at[d - 1], z_s, z_r, dev(z_=to_z))
        wait(rz, z_r)
        rows = qz[zl, zh]
        for i in range(7):
            rows += rz[i]
        gh[x] = rows

        for d in FAR:
            send(gh.at[x], gh.at[x], g_s, g_r, dev(x_=ahead(x, d, NX)))
        others = gh.at[pl.ds(0, 7)]
        wait(others, g_r)

        g = gh[...].reshape(128, HD)
        partial = lax.dot_general(
            g, g, (((0,), (0,)), ((), ())), precision=lax.Precision.HIGHEST, preferred_element_type=jnp.float32
        )
        af[...] = partial.reshape(8, 16, HD)

        send(af.at[x], rc, c_s, c_r, dev(z_=z + 1 - 2 * zl))
        wait(rc, c_r)
        pl.semaphore_signal(go_sem, inc=1, device_id=partner, device_id_type=MESH)
        bslice[...] = af[x] + rc[...]

        for d in FAR:
            send(bslice, rg.at[d - 1], b_s, b_r, dev(y_=ahead(y, d, NY)))
        wait(rg, b_r)
        total = bslice[...]
        for i in range(7):
            total += rg[i]
        gram[x] = total

        for d in FAR:
            send(gram.at[x], gram.at[x], a_s, a_r, dev(x_=ahead(x, d, NX)))
        wait(others, a_r)

        a = gram[...].reshape(HD, HD)
        row = lax.broadcasted_iota(jnp.int32, (HD, HD), 0)
        col = lax.broadcasted_iota(jnp.int32, (HD, HD), 1)
        eye = row == col
        identity = jnp.where(eye, 1.0, 0.0).astype(jnp.float32)
        square = jnp.sum(jnp.where(eye, a, 0.0), axis=0, keepdims=True)
        square = jnp.sum(square, axis=1, keepdims=True)
        divisor = jnp.sqrt(square) + epsilon
        a = a / (divisor * divisor)
        total = None
        for step in range(NS_ITERS):
            factor = coef_a * identity + coef_b * a + coef_c * mm(a, a)
            total = factor if total is None else mm(total, factor)
            if step + 1 < NS_ITERS:
                a = mm(factor, mm(a, factor))
        result = (0.2 * math.sqrt(DIN)) * mm(gh[...].reshape(128, HD) / divisor, total)
        result = result.astype(uz.dtype).reshape(2, 64, HD)
        uz[...] = result
        ub[zh] = result[1]

        for d in (2, 1, 3):
            send(uz.at[1], ub.at[zh], u_s, u_r, z_hi_peer(d, 1))
            send(uz.at[0], ub.at[zh], v_s, u_r, z_hi_peer(d, 0))
        send(uz.at[0], ub.at[zh], v_s, u_r, partner)

        wait(wfull, w3_r)
        finish()
        to_partner.wait_send()
        for like, sem in (
            (rx, x1_s), (ry, y1_s), (r2x, y2_s), (r2y, x2_s), (rz, z_s),
            (others, g_s), (rc, c_s), (rg, b_s), (others, a_s),
        ):
            wait(like, sem)
        three = ub.at[pl.ds(0, 3)]
        wait(three, u_r)
        place()
        wait(three, u_s)
        wait(ub, v_s)


def per_device(tokens, cotangent, value_weight):
    bf16, f32 = jnp.bfloat16, jnp.float32
    vmem, dma = pltpu.VMEM, pltpu.SemaphoreType.DMA
    args = tokens, cotangent, value_weight.reshape(NZH, 16, 512)
    return pl.pallas_call(
        kernel,
        out_shape=(
            jax.ShapeDtypeStruct((256, DIN), bf16),
            jax.ShapeDtypeStruct((64, 512), f32),
        ),
        in_specs=[pl.BlockSpec(memory_space=pltpu.HBM)] * 3,
        out_specs=(pl.BlockSpec(memory_space=pltpu.VMEM), pl.BlockSpec(memory_space=pltpu.VMEM)),
        scratch_shapes=[
            vmem((256, DIN), bf16),
            vmem((256, 512), bf16),
            vmem((2, NY, 2, NZH, 16, 512), bf16),
            vmem((16, 512), bf16),
            vmem((8, 2, 8, 16, 512), bf16),
            vmem((8, 2, 8, 16, 512), bf16),
            vmem((8, 8, 2, 16, 256), bf16),
            vmem((8, 2, 8, 16, 256), bf16),
            vmem((7, 8, 2, 16, 256), bf16),
            vmem((7, 2, 8, 16, 256), bf16),
            vmem((8, 2, 16, 256), bf16),
            vmem((8, 2, 16, 256), bf16),
            vmem((7, 2, 16, 256), bf16),
            vmem((7, 2, 16, 256), bf16),
            vmem((2, 4, 16, HD), f32),
            vmem((7, 16, HD), f32),
            vmem((8, 16, HD), f32),
            vmem((8, 16, HD), f32),
            vmem((16, HD), f32),
            vmem((16, HD), f32),
            vmem((7, 16, HD), f32),
            vmem((8, 16, HD), f32),
            vmem((4, 64, HD), UPDATE_DTYPE),
            vmem((2, 64, HD), UPDATE_DTYPE),
            dma((6,)), dma, dma((4,)), dma, dma, dma, dma, dma((2,)), dma((2,)), dma, dma,
            *[dma] * 12, *[dma] * 6, dma, dma, dma, pltpu.SemaphoreType.REGULAR,
        ],
        compiler_params=pltpu.CompilerParams(
            collective_id=0, has_side_effects=True, vmem_limit_bytes=VMEM_LIMIT
        ),
        name="whole",
    )(*(pltpu.with_memory_space_constraint(a, pltpu.HBM) for a in args))


def solution(mesh):
    in_specs = (P(("node", "rep"), None), P(("node", "rep"), None), P("node", None))
    out_specs = (P(("node", "rep"), None), P("node", None))
    return jax.shard_map(
        per_device, mesh=mesh, in_specs=in_specs, out_specs=out_specs, check_vma=False
    )
```

```python
import functools
import math

import jax
import jax.numpy as jnp
from jax import lax
from jax.experimental import pallas as pl
from jax.experimental.pallas import tpu as pltpu
from jax.sharding import PartitionSpec as P

MESH = pl.DeviceIdType.MESH

DIN = 2048
HD = 128
NS_ITERS = 5

coef_a = 3.4445
coef_b = -4.775
coef_c = 2.0315
epsilon = 1e-07

NX, NY, NZ, NZH = 8, 8, 8, 4
FAR = (4, 3, 5, 2, 6, 1, 7)
UPDATE_DTYPE = jnp.bfloat16
VMEM_LIMIT = 24 * 1024 * 1024


def split(a):
    parts, rest = [], a
    for _ in range(3):
        parts.append(rest.astype(jnp.bfloat16))
        rest = rest - parts[-1].astype(jnp.float32)
    p, q, r = parts
    left = jnp.concatenate([p, q], axis=1), jnp.concatenate([p, r], axis=1)
    right = (
        jnp.concatenate([jnp.concatenate([p, q], axis=1), jnp.concatenate([q, p], axis=1)], axis=0),
        jnp.concatenate([r, p], axis=0),
    )
    return left, right


def mm(a, b):
    (pq, pr), _ = a
    _, (square, rp) = b
    main = jnp.dot(pq, square, preferred_element_type=jnp.float32)
    return main[:, :HD] + (main[:, HD:] + jnp.dot(pr, rp, preferred_element_type=jnp.float32))


def kernel(
    tok_hbm, cot_hbm, w_hbm, ig_ref, up_ref,
    tok, cot, wfull, wown,
    termx, termy, other, pxa, pxb, pya, pyb, zx, zr, rxa, rxb, ry, sx, sy, r2x, r2y,
    qz, rz, gh, af, rc, bslice, rg, gram, ub, uz,
    load_sem, d2d_s, d2d_r, w0_s, w0_r, w1_s, w1_r, w2_s, w2_r, w3_s, w3_r, zx_s, zx_r,
    x1_s, x1_r, y1a_s, y1b_s, y1_r, x2_s, x2_r, y2_s, y2_r, z_s, z_r, g_s, g_r,
    c_s, c_r, b_s, b_r, a_s, a_r, u_s, v_s, u_r,
):
    node, rep = lax.axis_index("node"), lax.axis_index("rep")
    core = lax.rem(node, 2)
    y = lax.rem(lax.div(node, 2), NY)
    zl = lax.div(node, 2 * NY)
    x, zh = lax.div(rep, NZH), lax.rem(rep, NZH)
    z = zh * 2 + zl

    def dev(x_=None, y_=None, z_=None, core_=None):
        to = {}
        if y_ is not None or z_ is not None or core_ is not None:
            low = zl if z_ is None else lax.rem(z_, 2)
            to["node"] = (low * NY + (y if y_ is None else y_)) * 2 + (core if core_ is None else core_)
        if x_ is not None or z_ is not None:
            to["rep"] = (x if x_ is None else x_) * NZH + (zh if z_ is None else lax.div(z_, 2))
        return to

    def ahead(at, d, n):
        return lax.rem(at + d, n)

    def describe(src, dst, ssem, rsem, to):
        return pltpu.make_async_remote_copy(
            src_ref=src, dst_ref=dst, send_sem=ssem, recv_sem=rsem, device_id=to, device_id_type=MESH
        )

    def send(src, dst, ssem, rsem, to):
        describe(src, dst, ssem, rsem, to).start()

    def wait(like, sem):
        pltpu.make_async_copy(like, like, sem).wait()

    partner = dev(core_=1 - core)

    load_cot = pltpu.make_async_copy(cot_hbm, cot, load_sem.at[0])
    load_cot.start()
    pairs = [lax.rem(lax.div(y, 2) + 2 + k, 4) for k in range(4)]
    for k in range(4):
        for lo in range(2):
            columns = pl.ds(pl.multiple_of(lo * 1024 + pairs[k] * 256, 256), 256)
            slot = pl.ds(lo * 1024 + k * 256, 256)
            pltpu.make_async_copy(tok_hbm.at[:, columns], tok.at[:, slot], load_sem.at[2 + k]).start()
    load_w = pltpu.make_async_copy(w_hbm.at[zh], wown, load_sem.at[1])
    load_w.start()

    barrier = pltpu.get_barrier_semaphore()

    def greet(to):
        pl.semaphore_signal(barrier, inc=1, device_id=to, device_id_type=MESH)

    def z_hi_peer(d, core_):
        return dev(z_=lax.rem(zh + d, NZH) * 2 + zl, core_=core_)

    for d in FAR:
        greet(dev(z_=ahead(z, d, NZ)))
        greet(dev(y_=ahead(y, d, NY)))
        greet(dev(y_=ahead(y, d, NY), core_=1 - core))

        @pl.when(core == 1)
        def _(d=d):
            greet(dev(x_=ahead(x, d, NX)))

        if d == 4:

            @pl.when(core == 0)
            def _():
                for e in (2, 1, 3):
                    greet(z_hi_peer(e, 1))

    greet(partner)

    def compute(k):
        wait(tok.at[:, pl.ds(0, 512)], load_sem.at[2 + k])
        for lo in range(2):
            t = lax.dot_general(
                tok[:, lo * 1024 + k * 256 : lo * 1024 + k * 256 + 256],
                cot[...],
                (((0,), (0,)), ((), ())),
                preferred_element_type=jnp.float32,
            )
            t = t.reshape(2, 8, 16, 512).astype(jnp.bfloat16)
            termx[2 * k : 2 * k + 2, lo] = t[..., :256]
            termy[2 * k : 2 * k + 2, lo] = t[..., 256:]

    def summed(term, b, lo):
        return term[b, lo] + other[b, lo]

    pair = dev(z_=z + 1 - 2 * zl)

    def piece(at):
        return wfull.at[lax.rem(at, 2), :, :, lax.div(at, 2)]

    def finish():
        for k in range(8):
            lo, b = k // 4, 2 * (k % 4)
            weight = wfull[lo, b : b + 2].reshape(256, 512)
            ig_ref[:, k * 256 : k * 256 + 256] = lax.dot_general(
                cot[...], weight, (((1,), (1,)), ((), ())), preferred_element_type=jnp.float32
            ).astype(jnp.bfloat16)

    def place():
        for h in range(4):
            up_ref[:, h * HD : h * HD + HD] = ub[h].astype(jnp.float32)

    to_partner = describe(wown, wfull.at[zl, y, 1, zh], w0_s, w0_r, partner)

    @pl.when(core == 0)
    def _():
        load_cot.wait()
        for k in range(4):
            compute(k)
            if k == 0:
                pl.semaphore_wait(barrier, 22)
            ys = pl.ds(2 * k, 2)
            send(termx.at[ys], other.at[ys], d2d_s, d2d_r.at[k], partner)
            if k == 0:
                load_w.wait()
                for d in FAR:
                    send(wown, wfull.at[zl, y, 0, zh], w1_s, w1_r, dev(y_=ahead(y, d, NY)))
        wfull[zl, y, 0, zh] = wown[...]

        for k in range(4):
            wait(other.at[pl.ds(2 * k, 2)], d2d_r.at[k])
            zx[k] = summed(termy, 2 * k + 1, 1 - zl)
            send(zx.at[k], zr.at[k], zx_s, zx_r.at[k], pair)
            for lo in range(2):
                pya[k, lo] = summed(termy, 2 * k, lo)
            at_y = 2 * pairs[k]
            send(pya.at[k], ry.at[lax.rem(at_y + NY + 7 - y, NY)], y1a_s, y1_r, dev(y_=at_y, core_=1))
            pyb[k] = summed(termy, 2 * k + 1, zl)
        sevenths = wfull.at[0, pl.ds(0, 7), :, 0]

        def hop(at, up, step):
            to_z = ahead(z, 1 if up else NZ - 1, NZ)
            k = 2 * step + (0 if up else 1)
            send(piece(at), piece(at), w2_s.at[0 if up else 1], w2_r.at[k], dev(z_=to_z))

        for k in range(4):
            if k == 2:
                to_partner.wait_recv()
                wait(sevenths, w1_r)
                hop(z, True, 0)
                hop(z, False, 0)
                send(piece(z), piece(z), w3_s, w3_r, partner)
            wait(zr.at[k], zx_r.at[k])
            pyb[k] = pyb[k] + zr[k]
            at_y = 2 * pairs[k] + 1
            send(pyb.at[k], ry.at[lax.rem(at_y + NY + 7 - y, NY), 0], y1b_s, y1_r, dev(y_=at_y, core_=1))

        for step in range(4):
            for up in (True, False) if step < 3 else (True,):
                at = lax.rem(z + (NZ - 1 - step if up else 1 + step), NZ)
                wait(piece(at), w2_r.at[2 * step + (0 if up else 1)])
                if step < (3 if up else 2):
                    hop(at, up, step + 1)
                send(piece(at), piece(at), w3_s, w3_r, partner)
        finish()
        wait(termx, d2d_s)
        wait(zx, zx_s)
        wait(pya, y1a_s)
        wait(pyb, y1b_s)
        wait(wfull.at[0, pl.ds(0, 7), 0, 0], w1_s)
        wait(wfull.at[0], w2_s.at[0])
        wait(wfull.at[0, :, :, pl.ds(0, 3)], w2_s.at[1])
        wait(wfull, w3_s)
        wait(ub, u_r)
        place()

    @pl.when(core == 1)
    def _():
        load_cot.wait()
        for k in range(4):
            compute(k)
            if k == 0:
                pl.semaphore_wait(barrier, 32)
            ys = pl.ds(2 * k, 2)
            send(termy.at[ys], other.at[ys], d2d_s, d2d_r.at[k], partner)
            if k == 0:
                load_w.wait()
                to_partner.start()
                for d in FAR:
                    send(wown, wfull.at[zl, y, 1, zh], w1_s, w1_r, dev(y_=ahead(y, d, NY), core_=0))

        for k in range(4):
            wait(other.at[pl.ds(2 * k, 2)], d2d_r.at[k])
            zx[k] = summed(termx, 2 * k + 1, 1 - zl)
            send(zx.at[k], zr.at[k], zx_s, zx_r.at[k], pair)
            for lo in range(2):
                pxa[:, k, lo] = summed(termx, 2 * k, lo)
            pxb[:, k] = summed(termx, 2 * k + 1, zl)
            if k % 2 == 1:
                ks = pl.ds(k - 1, 2)
                for d in FAR:
                    to_x = ahead(x, d, NX)
                    send(pxa.at[to_x, ks], rxa.at[d - 1, ks], x1_s.at[0], x1_r.at[0], dev(x_=to_x))
        for k in range(4):
            wait(zr.at[k], zx_r.at[k])
            pxb[:, k] = pxb[:, k] + zr[k]
            if k % 2 == 1:
                ks = pl.ds(k - 1, 2)
                for d in FAR:
                    to_x = ahead(x, d, NX)
                    send(pxb.at[to_x, ks], rxb.at[d - 1, ks], x1_s.at[1], x1_r.at[1], dev(x_=to_x))

        def total_of(first, parts):
            total = first.astype(jnp.float32)
            for part in parts:
                total += part.astype(jnp.float32)
            return total

        def middle(odd):
            n = 1 if odd else 2
            wait(rxa, x1_r.at[0])
            for k in range(4):
                for lo in range(2):
                    total = total_of(pxa[x, k, lo], [rxa[i, k, lo] for i in range(7)])
                    sx[2 * pairs[k], lo] = total.astype(jnp.bfloat16)
            wait(rxb, x1_r.at[1])
            for k in range(4):
                total = total_of(pxb[x, k], [rxb[i, k] for i in range(7)])
                sx[2 * pairs[k] + 1, 0] = total.astype(jnp.bfloat16)
            for d in FAR:
                to_y, m = ahead(y, d, NY), 1 if (d + odd) % 2 else 2
                part = pl.ds(0, m)
                send(sx.at[to_y, part], r2x.at[d - 1, part], y2_s.at[d % 2], y2_r, dev(y_=to_y))
            wait(ry.at[:, pl.ds(0, n)], y1_r)
            for b in range(8):
                for lo in range(n):
                    total = total_of(ry[7, lo, b], [ry[i, lo, b] for i in range(7)])
                    sy[b, lo] = total.astype(jnp.bfloat16)
            part = pl.ds(0, n)
            for d in FAR:
                to_x = ahead(x, d, NX)
                send(sy.at[to_x, part], r2y.at[d - 1, part], x2_s, x2_r, dev(x_=to_x))
            wait(r2x.at[:, part], y2_r)
            wait(r2y.at[:, part], x2_r)
            for lo in range(n):
                total_x = total_of(sx[y, lo], [r2x[i, lo] for i in range(7)])
                total_y = total_of(sy[x, lo], [r2y[i, lo] for i in range(7)])
                for h in range(4):
                    source = total_x if h < 2 else total_y
                    qz[lo, h] = source[:, (h % 2) * HD : (h % 2) * HD + HD]
            if odd:
                for d in (2, 1, 3):
                    to_h = lax.rem(zh + d, NZH)
                    send(qz.at[0, to_h], rz.at[d - 1], z_s, z_r, z_hi_peer(d, 1))
                slots = 3
            else:
                for d in FAR:
                    to_z = ahead(z, d, NZ)
                    send(qz.at[lax.rem(to_z, 2), lax.div(to_z, 2)], rz.at[d - 1], z_s, z_r, dev(z_=to_z))
                slots = 7
            wait(rz.at[pl.ds(0, slots)], z_r)
            rows = qz[0 if odd else zl, zh]
            for i in range(slots):
                rows += rz[i]
            gh[x] = rows
            wait(r2x.at[pl.ds(0, 4), pl.ds(0, 2 if odd else 1)], y2_s.at[1])
            wait(r2x.at[pl.ds(0, 3), pl.ds(0, 1 if odd else 2)], y2_s.at[0])
            wait(r2y.at[:, part], x2_s)
            wait(rz.at[pl.ds(0, slots)], z_s)

        odd_y = lax.rem(y, 2)

        @pl.when(odd_y == 0)
        def _():
            middle(0)

        @pl.when(odd_y == 1)
        def _():
            middle(1)

        for d in FAR:
            send(gh.at[x], gh.at[x], g_s, g_r, dev(x_=ahead(x, d, NX)))
        others = gh.at[pl.ds(0, 7)]
        wait(others, g_r)

        g = gh[...].reshape(128, HD)
        partial = lax.dot_general(
            g, g, (((0,), (0,)), ((), ())), precision=lax.Precision.HIGHEST, preferred_element_type=jnp.float32
        )
        af[...] = partial.reshape(8, 16, HD)

        send(af.at[x], rc, c_s, c_r, pair)
        wait(rc, c_r)
        bslice[...] = af[x] + rc[...]

        for d in FAR:
            send(bslice, rg.at[d - 1], b_s, b_r, dev(y_=ahead(y, d, NY)))
        wait(rg, b_r)
        total = bslice[...]
        for i in range(7):
            total += rg[i]
        gram[x] = total

        for d in FAR:
            send(gram.at[x], gram.at[x], a_s, a_r, dev(x_=ahead(x, d, NX)))
        wait(others, a_r)

        a = gram[...].reshape(HD, HD)
        row = lax.broadcasted_iota(jnp.int32, (HD, HD), 0)
        col = lax.broadcasted_iota(jnp.int32, (HD, HD), 1)
        eye = row == col
        identity = jnp.where(eye, 1.0, 0.0).astype(jnp.float32)
        square = jnp.sum(jnp.where(eye, a, 0.0), axis=0, keepdims=True)
        square = jnp.sum(square, axis=1, keepdims=True)
        divisor = jnp.sqrt(square) + epsilon
        a = a / (divisor * divisor)
        total = None
        for step in range(NS_ITERS):
            parts = split(a)
            factor = coef_a * identity + coef_b * a + coef_c * mm(parts, parts)
            f = split(factor)
            total = factor if total is None else mm(split(total), f)
            if step + 1 < NS_ITERS:
                a = mm(f, split(mm(parts, f)))
        result = (0.2 * math.sqrt(DIN)) * mm(split(gh[...].reshape(128, HD) / divisor), split(total))
        result = result.astype(uz.dtype).reshape(2, 64, HD)
        uz[...] = result
        ub[zh] = result[1]

        for d in (2, 1, 3):
            send(uz.at[1], ub.at[zh], u_s, u_r, z_hi_peer(d, 1))
            send(uz.at[0], ub.at[zh], v_s, u_r, z_hi_peer(d, 0))
        send(uz.at[0], ub.at[zh], v_s, u_r, partner)

        wait(wfull, w3_r)
        finish()
        to_partner.wait_send()
        for like, sem in (
            (termy, d2d_s), (zx, zx_s), (wfull.at[0, pl.ds(0, 7), 0, 0], w1_s),
            (rxa, x1_s.at[0]), (rxb, x1_s.at[1]),
            (others, g_s), (rc, c_s), (rg, b_s), (others, a_s),
        ):
            wait(like, sem)
        three = ub.at[pl.ds(0, 3)]
        wait(three, u_r)
        place()
        wait(three, u_s)
        wait(ub, v_s)


def store(ig_ref, up_ref, ig_hbm, up_hbm, sems):
    copies = [
        pltpu.make_async_copy(ig_ref.at[pl.ds(64 * k, 64)], ig_hbm.at[pl.ds(64 * k, 64)], sems.at[k]) for k in range(4)
    ]
    copies.append(pltpu.make_async_copy(up_ref, up_hbm, sems.at[4]))
    for copy in copies:
        copy.start()
    for copy in copies:
        copy.wait()


def per_device(tokens, cotangent, value_weight):
    bf16, f32 = jnp.bfloat16, jnp.float32
    vmem, dma = pltpu.VMEM, pltpu.SemaphoreType.DMA
    args = tokens, cotangent, value_weight.reshape(NZH, 16, 512)
    results = pl.pallas_call(
        kernel,
        out_shape=(
            jax.ShapeDtypeStruct((256, DIN), bf16),
            jax.ShapeDtypeStruct((64, 512), f32),
        ),
        in_specs=[pl.BlockSpec(memory_space=pltpu.HBM)] * 3,
        out_specs=(pl.BlockSpec(memory_space=pltpu.VMEM), pl.BlockSpec(memory_space=pltpu.VMEM)),
        scratch_shapes=[
            vmem((256, DIN), bf16),
            vmem((256, 512), bf16),
            vmem((2, NY, 2, NZH, 16, 512), bf16),
            vmem((16, 512), bf16),
            vmem((8, 2, 8, 16, 256), bf16),
            vmem((8, 2, 8, 16, 256), bf16),
            vmem((8, 2, 8, 16, 256), bf16),
            vmem((8, 4, 2, 16, 256), bf16),
            vmem((8, 4, 16, 256), bf16),
            vmem((4, 2, 8, 16, 256), bf16),
            vmem((4, 8, 16, 256), bf16),
            vmem((4, 8, 16, 256), bf16),
            vmem((4, 8, 16, 256), bf16),
            vmem((7, 4, 2, 16, 256), bf16),
            vmem((7, 4, 16, 256), bf16),
            vmem((8, 2, 8, 16, 256), bf16),
            vmem((8, 2, 16, 256), bf16),
            vmem((8, 2, 16, 256), bf16),
            vmem((7, 2, 16, 256), bf16),
            vmem((7, 2, 16, 256), bf16),
            vmem((2, 4, 16, HD), f32),
            vmem((7, 16, HD), f32),
            vmem((8, 16, HD), f32),
            vmem((8, 16, HD), f32),
            vmem((16, HD), f32),
            vmem((16, HD), f32),
            vmem((7, 16, HD), f32),
            vmem((8, 16, HD), f32),
            vmem((4, 64, HD), UPDATE_DTYPE),
            vmem((2, 64, HD), UPDATE_DTYPE),
            dma((6,)), dma, dma((4,)), dma, dma, dma, dma, dma((2,)), dma((7,)), dma, dma, dma, dma((4,)),
            dma((2,)), dma((2,)), dma, dma, dma, dma, dma, dma((2,)), dma, *[dma] * 4,
            *[dma] * 6, dma, dma, dma,
        ],
        compiler_params=pltpu.CompilerParams(
            collective_id=0, has_side_effects=True, vmem_limit_bytes=VMEM_LIMIT
        ),
        name="whole",
    )(*(pltpu.with_memory_space_constraint(a, pltpu.HBM) for a in args))
    return pl.pallas_call(
        store,
        out_shape=(
            jax.ShapeDtypeStruct((256, DIN), bf16),
            jax.ShapeDtypeStruct((64, 512), f32),
        ),
        in_specs=[pl.BlockSpec(memory_space=pltpu.VMEM)] * 2,
        out_specs=(pl.BlockSpec(memory_space=pltpu.HBM), pl.BlockSpec(memory_space=pltpu.HBM)),
        scratch_shapes=[dma((5,))],
        compiler_params=pltpu.CompilerParams(vmem_limit_bytes=8 * 1024 * 1024),
        name="store",
    )(*results)


def solution(mesh):
    in_specs = (P(("node", "rep"), None), P(("node", "rep"), None), P("node", None))
    out_specs = (P(("node", "rep"), None), P("node", None))
    return jax.shard_map(
        per_device, mesh=mesh, in_specs=in_specs, out_specs=out_specs, check_vma=False
    )
```

```python
import functools
import math

import jax
import jax.numpy as jnp
from jax import lax
from jax.experimental import pallas as pl
from jax.experimental.pallas import tpu as pltpu
from jax.sharding import PartitionSpec as P

MESH = pl.DeviceIdType.MESH

DIN = 2048
HD = 128
NS_ITERS = 5

coef_a = 3.4445
coef_b = -4.775
coef_c = 2.0315
epsilon = 1e-07

NX, NY, NZ, NZH = 8, 8, 8, 4
FAR = (4, 3, 5, 2, 6, 1, 7)
UPDATE_DTYPE = jnp.bfloat16
VMEM_LIMIT = 24 * 1024 * 1024


def split(a):
    parts, rest = [], a
    for _ in range(3):
        parts.append(rest.astype(jnp.bfloat16))
        rest = rest - parts[-1].astype(jnp.float32)
    p, q, r = parts
    left = jnp.concatenate([p, q], axis=1), jnp.concatenate([p, r], axis=1)
    right = (
        jnp.concatenate([jnp.concatenate([p, q], axis=1), jnp.concatenate([q, p], axis=1)], axis=0),
        jnp.concatenate([r, p], axis=0),
    )
    return left, right


def mm(a, b):
    (pq, pr), _ = a
    _, (square, rp) = b
    main = jnp.dot(pq, square, preferred_element_type=jnp.float32)
    return main[:, :HD] + (main[:, HD:] + jnp.dot(pr, rp, preferred_element_type=jnp.float32))


def kernel(
    tok_hbm, cot_hbm, w_hbm, ig_ref, up_ref,
    tok, cot, wfull, wown,
    termx, termy, other, pxa, pxb, pya, pyb, zx, zr, fxa, fya, rxa, rxb, ry, sx, sy, r2x, r2y,
    qz, rz, gh, af, rg, gram, ub, uz,
    load_sem, d2d_s, d2d_r, w0_s, w0_r, w1_s, w1_r, w2_s, w2_r, w3_s, w3_r, zx_s, zx_r, f_s, f_r,
    x1_s, x1_r, y1a_s, y1b_s, y1_r, x2_s, x2_r, y2_s, y2_r, z_s, z_r, g_s, g_r,
    b_s, b_r, a_s, a_r, u_s, v_s, u_r,
):
    node, rep = lax.axis_index("node"), lax.axis_index("rep")
    core = lax.rem(node, 2)
    y = lax.rem(lax.div(node, 2), NY)
    zl = lax.div(node, 2 * NY)
    x, zh = lax.div(rep, NZH), lax.rem(rep, NZH)
    z = zh * 2 + zl

    def dev(x_=None, y_=None, z_=None, core_=None):
        to = {}
        if y_ is not None or z_ is not None or core_ is not None:
            low = zl if z_ is None else lax.rem(z_, 2)
            to["node"] = (low * NY + (y if y_ is None else y_)) * 2 + (core if core_ is None else core_)
        if x_ is not None or z_ is not None:
            to["rep"] = (x if x_ is None else x_) * NZH + (zh if z_ is None else lax.div(z_, 2))
        return to

    def ahead(at, d, n):
        return lax.rem(at + d, n)

    def describe(src, dst, ssem, rsem, to):
        return pltpu.make_async_remote_copy(
            src_ref=src, dst_ref=dst, send_sem=ssem, recv_sem=rsem, device_id=to, device_id_type=MESH
        )

    def send(src, dst, ssem, rsem, to):
        describe(src, dst, ssem, rsem, to).start()

    def wait(like, sem):
        pltpu.make_async_copy(like, like, sem).wait()

    partner = dev(core_=1 - core)

    load_cot = pltpu.make_async_copy(cot_hbm, cot, load_sem.at[0])
    load_cot.start()
    pairs = [lax.rem(lax.div(y, 2) + 2 + k, 4) for k in range(4)]
    for k in range(4):
        for lo in range(2):
            columns = pl.ds(pl.multiple_of(lo * 1024 + pairs[k] * 256, 256), 256)
            slot = pl.ds(lo * 1024 + k * 256, 256)
            pltpu.make_async_copy(tok_hbm.at[:, columns], tok.at[:, slot], load_sem.at[2 + k]).start()
    load_w = pltpu.make_async_copy(w_hbm.at[zh], wown, load_sem.at[1])
    load_w.start()

    barrier = pltpu.get_barrier_semaphore()

    def greet(to):
        pl.semaphore_signal(barrier, inc=1, device_id=to, device_id_type=MESH)

    def z_hi_peer(d, core_):
        return dev(z_=lax.rem(zh + d, NZH) * 2 + zl, core_=core_)

    for d in FAR:
        greet(dev(z_=ahead(z, d, NZ)))
        greet(dev(y_=ahead(y, d, NY)))
        greet(dev(y_=ahead(y, d, NY), core_=1 - core))

        @pl.when(core == 1)
        def _(d=d):
            greet(dev(x_=ahead(x, d, NX)))

    greet(partner)

    def compute(k):
        wait(tok.at[:, pl.ds(0, 512)], load_sem.at[2 + k])
        for lo in range(2):
            t = lax.dot_general(
                tok[:, lo * 1024 + k * 256 : lo * 1024 + k * 256 + 256],
                cot[...],
                (((0,), (0,)), ((), ())),
                preferred_element_type=jnp.float32,
            )
            t = t.reshape(2, 8, 16, 512).astype(jnp.bfloat16)
            termx[2 * k : 2 * k + 2, lo] = t[..., :256]
            termy[2 * k : 2 * k + 2, lo] = t[..., 256:]

    def summed(term, b, lo):
        return term[b, lo] + other[b, lo]

    pair = dev(z_=z + 1 - 2 * zl)

    def piece(at):
        return wfull.at[lax.rem(at, 2), :, :, lax.div(at, 2)]

    def finish():
        for k in range(8):
            lo, b = k // 4, 2 * (k % 4)
            weight = wfull[lo, b : b + 2].reshape(256, 512)
            ig_ref[:, k * 256 : k * 256 + 256] = lax.dot_general(
                cot[...], weight, (((1,), (1,)), ((), ())), preferred_element_type=jnp.float32
            ).astype(jnp.bfloat16)

    def place():
        for h in range(4):
            up_ref[:, h * HD : h * HD + HD] = ub[h].astype(jnp.float32)

    to_partner = describe(wown, wfull.at[zl, y, 1, zh], w0_s, w0_r, partner)

    odd_y = lax.rem(y, 2)

    def whole_rows(k, odd):
        d = ((4, 6, 0, 2), (3, 5, 7, 1))[odd][k]

        @pl.when(odd_y == odd)
        def _():
            if d == 4:
                send(pya.at[k], fya, f_s.at[1], f_r.at[2], dev(y_=ahead(y, NY - 1, NY)))
            elif d != 5:
                send(pya.at[k], ry.at[(d + 7) % 8], y1a_s, y1_r, dev(y_=2 * pairs[k], core_=1))

    behind = dev(x_=ahead(x, NX - 1, NX))
    x5 = ahead(x, 5, NX)

    @pl.when(core == 0)
    def _():
        load_cot.wait()
        for k in range(4):
            compute(k)
            if k == 0:
                pl.semaphore_wait(barrier, 22)
            ys = pl.ds(2 * k, 2)
            send(termx.at[ys], other.at[ys], d2d_s, d2d_r.at[k], partner)
            if k == 0:
                load_w.wait()
                for d in FAR:
                    send(wown, wfull.at[zl, y, 0, zh], w1_s, w1_r, dev(y_=ahead(y, d, NY)))
        wfull[zl, y, 0, zh] = wown[...]

        for k in range(4):
            wait(other.at[pl.ds(2 * k, 2)], d2d_r.at[k])
            zx[k] = summed(termy, 2 * k + 1, 1 - zl)
            send(zx.at[k], zr.at[k], zx_s, zx_r.at[k], pair)
            for lo in range(2):
                pya[k, lo] = summed(termy, 2 * k, lo)
            whole_rows(k, 0)
            whole_rows(k, 1)
            pyb[k] = summed(termy, 2 * k + 1, zl)
        sevenths = wfull.at[0, pl.ds(0, 7), :, 0]

        def hop(at, up, step):
            to_z = ahead(z, 1 if up else NZ - 1, NZ)
            k = 2 * step + (0 if up else 1)
            send(piece(at), piece(at), w2_s.at[0 if up else 1], w2_r.at[k], dev(z_=to_z))

        for k in range(4):
            if k == 2:
                to_partner.wait_recv()
                wait(sevenths, w1_r)
                hop(z, True, 0)
                hop(z, False, 0)
                send(piece(z), piece(z), w3_s, w3_r, partner)
            wait(zr.at[k], zx_r.at[k])
            pyb[k] = pyb[k] + zr[k]
            at_y = 2 * pairs[k] + 1
            send(pyb.at[k], ry.at[lax.rem(at_y + NY + 7 - y, NY), 0], y1b_s, y1_r, dev(y_=at_y, core_=1))
            if k == 1:

                @pl.when(odd_y == 1)
                def _():
                    wait(fya, f_r.at[2])
                    pya[1] = pya[1] + fya[...]
                    send(pya.at[1], ry.at[4], y1a_s, y1_r, dev(y_=2 * pairs[1], core_=1))

        for step in range(4):
            for up in (True, False) if step < 3 else (True,):
                at = lax.rem(z + (NZ - 1 - step if up else 1 + step), NZ)
                wait(piece(at), w2_r.at[2 * step + (0 if up else 1)])
                if step < (3 if up else 2):
                    hop(at, up, step + 1)
                send(piece(at), piece(at), w3_s, w3_r, partner)
        finish()
        wait(termx, d2d_s)
        wait(zx, zx_s)

        @pl.when(odd_y == 0)
        def _():
            wait(pya.at[pl.ds(0, 3)], y1a_s)
            wait(fya, f_s.at[1])

        @pl.when(odd_y == 1)
        def _():
            wait(pya, y1a_s)

        wait(pyb, y1b_s)
        wait(wfull.at[0, pl.ds(0, 7), 0, 0], w1_s)
        wait(wfull.at[0], w2_s.at[0])
        wait(wfull.at[0, :, :, pl.ds(0, 3)], w2_s.at[1])
        wait(wfull, w3_s)
        wait(ub, u_r)
        place()

    @pl.when(core == 1)
    def _():
        load_cot.wait()
        for k in range(4):
            compute(k)
            if k == 0:
                pl.semaphore_wait(barrier, 29)
            ys = pl.ds(2 * k, 2)
            send(termy.at[ys], other.at[ys], d2d_s, d2d_r.at[k], partner)
            if k == 0:
                load_w.wait()
                to_partner.start()
                for d in FAR:
                    send(wown, wfull.at[zl, y, 1, zh], w1_s, w1_r, dev(y_=ahead(y, d, NY), core_=0))

        for k in range(4):
            wait(other.at[pl.ds(2 * k, 2)], d2d_r.at[k])
            zx[k] = summed(termx, 2 * k + 1, 1 - zl)
            send(zx.at[k], zr.at[k], zx_s, zx_r.at[k], pair)
            for lo in range(2):
                pxa[:, k, lo] = summed(termx, 2 * k, lo)
            pxb[:, k] = summed(termx, 2 * k + 1, zl)
            if k % 2 == 1:
                ks = pl.ds(k - 1, 2)
                send(pxa.at[ahead(x, 4, NX), ks], fxa.at[ks], f_s.at[0], f_r.at[k // 2], behind)
                for d in (3, 2, 6, 1, 7):
                    to_x, at = ahead(x, d, NX), d - 1 if d < 4 else d - 2
                    send(pxa.at[to_x, ks], rxa.at[at, ks], x1_s.at[0], x1_r.at[0], dev(x_=to_x))
        for k in range(4):
            wait(zr.at[k], zx_r.at[k])
            pxb[:, k] = pxb[:, k] + zr[k]
            if k == 0:
                for j in range(2):
                    ks = pl.ds(2 * j, 2)
                    wait(fxa.at[ks], f_r.at[j])
                    pxa[x5, 2 * j : 2 * j + 2] = pxa[x5, 2 * j : 2 * j + 2] + fxa[2 * j : 2 * j + 2]
                    send(pxa.at[x5, ks], rxa.at[3, ks], x1_s.at[0], x1_r.at[0], dev(x_=x5))
            if k >= 1:
                ks = pl.ds(0, 2) if k == 1 else pl.ds(k, 1)
                for d in FAR:
                    to_x = ahead(x, d, NX)
                    send(pxb.at[to_x, ks], rxb.at[d - 1, ks], x1_s.at[1], x1_r.at[1], dev(x_=to_x))

        def total_of(first, parts):
            total = first.astype(jnp.float32)
            for part in parts:
                total += part.astype(jnp.float32)
            return total

        def middle(odd):
            n = 1 if odd else 2
            wait(rxa, x1_r.at[0])
            for k in range(4):
                for lo in range(2):
                    total = total_of(pxa[x, k, lo], [rxa[i, k, lo] for i in range(6)])
                    sx[2 * pairs[k], lo] = total.astype(jnp.bfloat16)
            wait(rxb, x1_r.at[1])
            for k in range(4):
                total = total_of(pxb[x, k], [rxb[i, k] for i in range(7)])
                sx[2 * pairs[k] + 1, 0] = total.astype(jnp.bfloat16)
            for d in FAR:
                to_y, m = ahead(y, d, NY), 1 if (d + odd) % 2 else 2
                part = pl.ds(0, m)
                send(sx.at[to_y, part], r2x.at[d - 1, part], y2_s.at[d % 2], y2_r, dev(y_=to_y))
            wait(ry.at[:, pl.ds(0, 1)] if odd else ry.at[pl.ds(0, 7)], y1_r)
            for b in range(8):
                for lo in range(n):
                    total = total_of(ry[7, lo, b], [ry[i, lo, b] for i in range(7) if odd or i != 3])
                    sy[b, lo] = total.astype(jnp.bfloat16)
            part = pl.ds(0, n)
            for d in FAR:
                to_x = ahead(x, d, NX)
                send(sy.at[to_x, part], r2y.at[d - 1, part], x2_s, x2_r, dev(x_=to_x))
            wait(r2x.at[:, part], y2_r)
            wait(r2y.at[:, part], x2_r)
            for lo in range(n):
                total_x = total_of(sx[y, lo], [r2x[i, lo] for i in range(7)])
                total_y = total_of(sy[x, lo], [r2y[i, lo] for i in range(7)])
                for h in range(4):
                    source = total_x if h < 2 else total_y
                    qz[lo, h] = source[:, (h % 2) * HD : (h % 2) * HD + HD]
            if odd:
                for d in (2, 1, 3):
                    to_h = lax.rem(zh + d, NZH)
                    send(qz.at[0, to_h], rz.at[d - 1], z_s, z_r, z_hi_peer(d, 1))
                slots = 3
            else:
                for d in FAR:
                    to_z = ahead(z, d, NZ)
                    send(qz.at[lax.rem(to_z, 2), lax.div(to_z, 2)], rz.at[d - 1], z_s, z_r, dev(z_=to_z))
                slots = 7
            wait(rz.at[pl.ds(0, slots)], z_r)
            rows = qz[0 if odd else zl, zh]
            for i in range(slots):
                rows += rz[i]
            gh[x] = rows
            wait(r2x.at[pl.ds(0, 4), pl.ds(0, 2 if odd else 1)], y2_s.at[1])
            wait(r2x.at[pl.ds(0, 3), pl.ds(0, 1 if odd else 2)], y2_s.at[0])
            wait(r2y.at[:, part], x2_s)
            wait(rz.at[pl.ds(0, slots)], z_s)

        @pl.when(odd_y == 0)
        def _():
            middle(0)

        @pl.when(odd_y == 1)
        def _():
            middle(1)

        for d in FAR:
            send(gh.at[x], gh.at[x], g_s, g_r, dev(x_=ahead(x, d, NX)))
        others = gh.at[pl.ds(0, 7)]
        wait(others, g_r)

        g = gh[...].reshape(128, HD)
        partial = lax.dot_general(
            g, g, (((0,), (0,)), ((), ())), precision=lax.Precision.HIGHEST, preferred_element_type=jnp.float32
        )
        af[...] = partial.reshape(8, 16, HD)

        for d in FAR:
            send(af.at[x], rg.at[d + 7], b_s, b_r, dev(y_=ahead(y, d, NY), z_=z + 1 - 2 * zl))
            send(af.at[x], rg.at[d - 1], b_s, b_r, dev(y_=ahead(y, d, NY)))
        send(af.at[x], rg.at[7], b_s, b_r, pair)
        wait(rg, b_r)
        total = af[x]
        for i in range(15):
            total += rg[i]
        gram[x] = total

        for d in FAR:
            send(gram.at[x], gram.at[x], a_s, a_r, dev(x_=ahead(x, d, NX)))
        wait(others, a_r)

        a = gram[...].reshape(HD, HD)
        row = lax.broadcasted_iota(jnp.int32, (HD, HD), 0)
        col = lax.broadcasted_iota(jnp.int32, (HD, HD), 1)
        eye = row == col
        identity = jnp.where(eye, 1.0, 0.0).astype(jnp.float32)
        square = jnp.sum(jnp.where(eye, a, 0.0), axis=0, keepdims=True)
        square = jnp.sum(square, axis=1, keepdims=True)
        divisor = jnp.sqrt(square) + epsilon
        a = a / (divisor * divisor)
        total = None
        for step in range(NS_ITERS):
            parts = split(a)
            factor = coef_a * identity + coef_b * a + coef_c * mm(parts, parts)
            f = split(factor)
            total = factor if total is None else mm(split(total), f)
            if step + 1 < NS_ITERS:
                a = mm(f, split(mm(parts, f)))
        result = (0.2 * math.sqrt(DIN)) * mm(split(gh[...].reshape(128, HD) / divisor), split(total))
        result = result.astype(uz.dtype).reshape(2, 64, HD)
        uz[...] = result
        ub[zh] = result[1]

        for d in (2, 1, 3):
            send(uz.at[1], ub.at[zh], u_s, u_r, z_hi_peer(d, 1))
            send(uz.at[0], ub.at[zh], v_s, u_r, z_hi_peer(d, 0))
        send(uz.at[0], ub.at[zh], v_s, u_r, partner)

        wait(wfull, w3_r)
        finish()
        to_partner.wait_send()
        for like, sem in (
            (termy, d2d_s), (zx, zx_s), (wfull.at[0, pl.ds(0, 7), 0, 0], w1_s),
            (rxa, x1_s.at[0]), (fxa, f_s.at[0]), (rxb, x1_s.at[1]),
            (others, g_s), (rg, b_s), (others, a_s),
        ):
            wait(like, sem)
        three = ub.at[pl.ds(0, 3)]
        wait(three, u_r)
        place()
        wait(three, u_s)
        wait(ub, v_s)


def store(ig_ref, up_ref, ig_hbm, up_hbm, sems):
    copies = [
        pltpu.make_async_copy(ig_ref.at[pl.ds(64 * k, 64)], ig_hbm.at[pl.ds(64 * k, 64)], sems.at[k]) for k in range(4)
    ]
    copies.append(pltpu.make_async_copy(up_ref, up_hbm, sems.at[4]))
    for copy in copies:
        copy.start()
    for copy in copies:
        copy.wait()


def per_device(tokens, cotangent, value_weight):
    bf16, f32 = jnp.bfloat16, jnp.float32
    vmem, dma = pltpu.VMEM, pltpu.SemaphoreType.DMA
    args = tokens, cotangent, value_weight.reshape(NZH, 16, 512)
    results = pl.pallas_call(
        kernel,
        out_shape=(
            jax.ShapeDtypeStruct((256, DIN), bf16),
            jax.ShapeDtypeStruct((64, 512), f32),
        ),
        in_specs=[pl.BlockSpec(memory_space=pltpu.HBM)] * 3,
        out_specs=(pl.BlockSpec(memory_space=pltpu.VMEM), pl.BlockSpec(memory_space=pltpu.VMEM)),
        scratch_shapes=[
            vmem((256, DIN), bf16),
            vmem((256, 512), bf16),
            vmem((2, NY, 2, NZH, 16, 512), bf16),
            vmem((16, 512), bf16),
            vmem((8, 2, 8, 16, 256), bf16),
            vmem((8, 2, 8, 16, 256), bf16),
            vmem((8, 2, 8, 16, 256), bf16),
            vmem((8, 4, 2, 16, 256), bf16),
            vmem((8, 4, 16, 256), bf16),
            vmem((4, 2, 8, 16, 256), bf16),
            vmem((4, 8, 16, 256), bf16),
            vmem((4, 8, 16, 256), bf16),
            vmem((4, 8, 16, 256), bf16),
            vmem((4, 2, 16, 256), bf16),
            vmem((2, 8, 16, 256), bf16),
            vmem((6, 4, 2, 16, 256), bf16),
            vmem((7, 4, 16, 256), bf16),
            vmem((8, 2, 8, 16, 256), bf16),
            vmem((8, 2, 16, 256), bf16),
            vmem((8, 2, 16, 256), bf16),
            vmem((7, 2, 16, 256), bf16),
            vmem((7, 2, 16, 256), bf16),
            vmem((2, 4, 16, HD), f32),
            vmem((7, 16, HD), f32),
            vmem((8, 16, HD), f32),
            vmem((8, 16, HD), f32),
            vmem((15, 16, HD), f32),
            vmem((8, 16, HD), f32),
            vmem((4, 64, HD), UPDATE_DTYPE),
            vmem((2, 64, HD), UPDATE_DTYPE),
            dma((6,)), dma, dma((4,)), dma, dma, dma, dma, dma((2,)), dma((7,)), dma, dma, dma, dma((4,)), dma((2,)), dma((3,)),
            dma((2,)), dma((2,)), dma, dma, dma, dma, dma, dma((2,)), dma, *[dma] * 4,
            *[dma] * 4, dma, dma, dma,
        ],
        compiler_params=pltpu.CompilerParams(
            collective_id=0, has_side_effects=True, vmem_limit_bytes=VMEM_LIMIT
        ),
        name="whole",
    )(*(pltpu.with_memory_space_constraint(a, pltpu.HBM) for a in args))
    return pl.pallas_call(
        store,
        out_shape=(
            jax.ShapeDtypeStruct((256, DIN), bf16),
            jax.ShapeDtypeStruct((64, 512), f32),
        ),
        in_specs=[pl.BlockSpec(memory_space=pltpu.VMEM)] * 2,
        out_specs=(pl.BlockSpec(memory_space=pltpu.HBM), pl.BlockSpec(memory_space=pltpu.HBM)),
        scratch_shapes=[dma((5,))],
        compiler_params=pltpu.CompilerParams(vmem_limit_bytes=8 * 1024 * 1024),
        name="store",
    )(*results)


def solution(mesh):
    in_specs = (P(("node", "rep"), None), P(("node", "rep"), None), P("node", None))
    out_specs = (P(("node", "rep"), None), P("node", None))
    return jax.shard_map(
        per_device, mesh=mesh, in_specs=in_specs, out_specs=out_specs, check_vma=False
    )
```
